8 devices in a mesh: dp: 4 (over z, y, x), pp: 2 (over core).
Axes of the slice: x: 2, y: 2, z: 1, core: 2. Of those that a mesh axis runs over, the one named last changes fastest.
Arguments:
- tokens: int32 [4, 12, 258], P(None, 'dp')
- emb_stack: float32 [2, 50304, 768], P('pp')
- w_up: bfloat16 [2, 1, 768, 3072], P('pp')
- w_down: bfloat16 [2, 1, 3072, 768], P('pp')
- gain_final: bfloat16 [768], replicated
- gain_hid: bfloat16 [768], replicated
- gain_emb: bfloat16 [768], replicated
- gain_mtp: bfloat16 [768], replicated
- w_proj: bfloat16 [1536, 768], replicated
- u_up: bfloat16 [768, 3072], replicated
- u_down: bfloat16 [3072, 768], replicated
- w_out: bfloat16 [768, 50304], replicated
Outputs:
- output 1: float32 [], replicated
- output 2: float32 [2, 50304, 768], P('pp')
- output 3: float32 [2, 1, 768, 3072], P('pp')
- output 4: float32 [2, 1, 3072, 768], P('pp')
All inputs are finite; a program needn't handle non-finite values.
Results may differ from the reference program's by a relative error of at most 0.0194833.
Values are sent between devices in bfloat16 or wider.
A program may use at most 1.75 GiB of HBM per device.

```python
import math
import jax
import jax.numpy as jnp
from jax import lax

STAGES = 2
REPLICAS = 4
VOCAB_SIZE = 50304
HIDDEN = 768
FFN_DIM = 3072
LAYERS = 1
MICRO_BATCHES = 4
BATCH_DEV = 3
SEQ_LEN = 256

BATCH = REPLICAS * BATCH_DEV
TOTAL_TOKENS = MICRO_BATCHES * BATCH * SEQ_LEN
NORM_EPS = 1e-6
MTP_WEIGHT = 0.3


def rms_plain(values):
    as_wide = values.astype(jnp.float32)
    inv_rms = lax.rsqrt(jnp.mean(as_wide * as_wide, axis=-1, keepdims=True) + NORM_EPS)
    return (as_wide * inv_rms).astype(jnp.bfloat16)


def rms_scale(values, gain_vec):
    as_wide = values.astype(jnp.float32)
    inv_rms = lax.rsqrt(jnp.mean(as_wide * as_wide, axis=-1, keepdims=True) + NORM_EPS)
    return (as_wide * inv_rms * gain_vec.astype(jnp.float32)).astype(jnp.bfloat16)


def mlp_tail(layer_in, normed, w_in, w_back):
    pre_act = jnp.dot(normed, w_in, preferred_element_type=jnp.float32)
    gelu_out = jax.nn.gelu(pre_act).astype(jnp.bfloat16)
    branch = jnp.dot(gelu_out, w_back, preferred_element_type=jnp.float32)
    return (layer_in.astype(jnp.float32) + branch).astype(jnp.bfloat16)


def token_xent(features, w_out, targets):
    logits = jnp.dot(features, w_out, preferred_element_type=jnp.float32)
    log_norm = jax.nn.logsumexp(logits, axis=-1)
    picked = jnp.take_along_axis(logits, targets[..., None], axis=-1)[..., 0]
    return jnp.sum(log_norm - picked)


def head_loss(hid_rows, nxt_rows, ids_rows, params, loss_scale):
    gain_final, gain_hid, gain_emb, gain_mtp, w_proj, u_up, u_down, w_out = params
    seq_len = hid_rows.shape[-2]
    main_sum = token_xent(rms_scale(hid_rows, gain_final), w_out, ids_rows[..., 1:seq_len + 1])
    joined = jnp.concatenate([rms_scale(hid_rows, gain_hid), rms_scale(nxt_rows, gain_emb)], axis=-1)
    mtp_in = jnp.dot(joined, w_proj, preferred_element_type=jnp.float32).astype(jnp.bfloat16)
    mtp_out = mlp_tail(mtp_in, rms_scale(mtp_in, gain_mtp), u_up, u_down)
    extra_sum = token_xent(rms_scale(mtp_out, gain_final), w_out, ids_rows[..., 2:seq_len + 2])
    return (main_sum + MTP_WEIGHT * extra_sum) * loss_scale


def row_loss(trunk_rows, next_rows, w_up, w_down, ids_row, params):
    flat_up = w_up.reshape(STAGES * LAYERS, HIDDEN, FFN_DIM)
    flat_down = w_down.reshape(STAGES * LAYERS, FFN_DIM, HIDDEN)

    def layer_step(layer_in, layer_w):
        return mlp_tail(layer_in, rms_plain(layer_in), layer_w[0], layer_w[1]), None

    hidden, _ = lax.scan(layer_step, trunk_rows, (flat_up, flat_down))
    return head_loss(hidden, next_rows, ids_row, params, 1.0 / TOTAL_TOKENS)


def setup_inputs(seed: int = 0) -> dict:
    key_list = jax.random.split(jax.random.key(seed), 12)
    tokens = jax.random.randint(key_list[0], (MICRO_BATCHES, BATCH, SEQ_LEN + 2), 0, VOCAB_SIZE, dtype=jnp.int32)
    tokens = tokens.at[0, 0, 0].set(VOCAB_SIZE - 1).at[0, 0, 1].set(0)
    emb_table = jax.random.normal(key_list[1], (VOCAB_SIZE, HIDDEN), jnp.float32)
    emb_stack = jnp.concatenate([emb_table[None], jnp.zeros((STAGES - 1, VOCAB_SIZE, HIDDEN), jnp.float32)])
    up_scale = 1.0 / math.sqrt(HIDDEN)
    down_scale = 2.0 / math.sqrt(FFN_DIM * STAGES * LAYERS)
    w_up = (jax.random.normal(key_list[2], (STAGES, LAYERS, HIDDEN, FFN_DIM), jnp.float32) * up_scale).astype(jnp.bfloat16)
    w_down = (jax.random.normal(key_list[3], (STAGES, LAYERS, FFN_DIM, HIDDEN), jnp.float32) * down_scale).astype(jnp.bfloat16)
    gain_final = (0.5 + jax.random.uniform(key_list[4], (HIDDEN,), jnp.float32)).astype(jnp.bfloat16)
    gain_hid = (0.5 + jax.random.uniform(key_list[5], (HIDDEN,), jnp.float32)).astype(jnp.bfloat16)
    gain_emb = (0.5 + jax.random.uniform(key_list[6], (HIDDEN,), jnp.float32)).astype(jnp.bfloat16)
    gain_mtp = (0.5 + jax.random.uniform(key_list[7], (HIDDEN,), jnp.float32)).astype(jnp.bfloat16)
    proj_scale = 1.0 / math.sqrt(2 * HIDDEN)
    w_proj = (jax.random.normal(key_list[8], (2 * HIDDEN, HIDDEN), jnp.float32) * proj_scale).astype(jnp.bfloat16)
    u_up = (jax.random.normal(key_list[9], (HIDDEN, FFN_DIM), jnp.float32) * up_scale).astype(jnp.bfloat16)
    u_down = (jax.random.normal(key_list[10], (FFN_DIM, HIDDEN), jnp.float32) / math.sqrt(FFN_DIM)).astype(jnp.bfloat16)
    w_out = (jax.random.normal(key_list[11], (HIDDEN, VOCAB_SIZE), jnp.float32) * (1.5 * up_scale)).astype(jnp.bfloat16)
    return {'tokens': tokens, 'emb_stack': emb_stack, 'w_up': w_up, 'w_down': w_down, 'gain_final': gain_final, 'gain_hid': gain_hid, 'gain_emb': gain_emb, 'gain_mtp': gain_mtp, 'w_proj': w_proj, 'u_up': u_up, 'u_down': u_down, 'w_out': w_out}


def reference(tokens, emb_stack, w_up, w_down, gain_final, gain_hid, gain_emb, gain_mtp, w_proj, u_up, u_down, w_out):
    params = (gain_final, gain_hid, gain_emb, gain_mtp, w_proj, u_up, u_down, w_out)
    emb_table = emb_stack[0]
    row_ids = tokens.reshape(MICRO_BATCHES * BATCH, SEQ_LEN + 2)
    grad_fn = jax.value_and_grad(row_loss, argnums=(0, 1, 2, 3))

    def row_step(acc_state, ids_row):
        loss_sum, acc_up, acc_down = acc_state
        trunk_rows = jnp.take(emb_table, ids_row[:SEQ_LEN], axis=0).astype(jnp.bfloat16)
        next_rows = jnp.take(emb_table, ids_row[1:SEQ_LEN + 1], axis=0).astype(jnp.bfloat16)
        row_value, row_grads = grad_fn(trunk_rows, next_rows, w_up, w_down, ids_row, params)
        new_state = (loss_sum + row_value, acc_up + row_grads[2].astype(jnp.float32), acc_down + row_grads[3].astype(jnp.float32))
        return new_state, (row_grads[0], row_grads[1])

    init_state = (jnp.zeros((), jnp.float32), jnp.zeros(w_up.shape, jnp.float32), jnp.zeros(w_down.shape, jnp.float32))
    final_state, row_outs = lax.scan(row_step, init_state, row_ids)
    total_loss, d_up, d_down = final_state
    d_trunk, d_next = row_outs
    all_ids = jnp.concatenate([row_ids[:, :SEQ_LEN].reshape(-1), row_ids[:, 1:SEQ_LEN + 1].reshape(-1)])
    all_rows = jnp.concatenate([d_trunk.reshape(-1, HIDDEN), d_next.reshape(-1, HIDDEN)]).astype(jnp.float32)
    d_table = jax.ops.segment_sum(all_rows, all_ids, num_segments=VOCAB_SIZE)
    d_stack = jnp.concatenate([d_table[None], jnp.zeros((STAGES - 1, VOCAB_SIZE, HIDDEN), jnp.float32)])
    return (total_loss, d_stack, d_up, d_down)
```

```python
import functools
import jax
import jax.numpy as jnp
from jax import lax
from jax.experimental import pallas as pl
from jax.experimental.pallas import tpu as pltpu
from jax.sharding import PartitionSpec as P

NORM_EPS = 1e-6
MTP_WEIGHT = 0.3
LOG2E = 1.4426950408889634
LN2 = 0.6931471805599453
VB = 1024
RC = 256
TAIL = 128
TB = 384
KW = 16
F32 = jnp.float32
BF16 = jnp.bfloat16


def rms_plain(values):
    as_wide = values.astype(F32)
    inv_rms = lax.rsqrt(jnp.mean(as_wide * as_wide, axis=-1, keepdims=True) + NORM_EPS)
    return (as_wide * inv_rms).astype(BF16)


def rms_scale(values, gain_vec):
    as_wide = values.astype(F32)
    inv_rms = lax.rsqrt(jnp.mean(as_wide * as_wide, axis=-1, keepdims=True) + NORM_EPS)
    return (as_wide * inv_rms * gain_vec.astype(F32)).astype(BF16)


def dot(a, b):
    return jnp.dot(a, b, preferred_element_type=F32)


def dot_nt(a, b):
    return lax.dot_general(a, b, (((1,), (1,)), ((), ())), preferred_element_type=F32)


def dot_tn(a, b):
    return lax.dot_general(a, b, (((0,), (0,)), ((), ())), preferred_element_type=F32)


def add_bf16(a, b):
    return (a.astype(F32) + b.astype(F32)).astype(BF16)


def mlp_forward(layer_in, normed, w_in, w_back):
    pre_act = dot(normed, w_in)
    gelu_out = jax.nn.gelu(pre_act).astype(BF16)
    out = (layer_in.astype(F32) + dot(gelu_out, w_back)).astype(BF16)
    return out, pre_act, gelu_out


def mlp_backward(grad_out, pre_act, w_in, w_back):
    grad_gelu = dot_nt(grad_out, w_back).astype(BF16)
    grad_pre = jax.vjp(jax.nn.gelu, pre_act)[1](grad_gelu.astype(F32))[0].astype(BF16)
    return grad_pre, dot_nt(grad_pre, w_in).astype(BF16)


def rank_of(ids):
    n = ids.shape[-1]
    key = ids * n + lax.iota(jnp.int32, n)
    return jnp.sum((key[..., None, :] < key[..., :, None]).astype(jnp.int32), axis=-1)


def sort_by_rank(ids, rank):
    n = ids.shape[-1]
    hit = rank[..., None, :] == lax.iota(jnp.int32, n)[:, None]
    return jnp.sum(jnp.where(hit, ids[..., None, :], 0), axis=-1)


def sort_rows(rows, rank):
    n = rank.shape[-1]
    hit = rank[None, :] == lax.iota(jnp.int32, n)[:, None]
    return dot(hit.astype(BF16), rows).astype(BF16)


def prep_kernel(info, ids, off, emb_ref, w_ref, wt_ref, tgt_ref, rows_ref, out_ref, buf, acc, sems, *, group, n_pad, n_blocks):
    step = pl.program_id(0)
    is_first = info[0] == 0

    @pl.when(is_first)
    def _():
        slot = lax.rem(step, 2)

        def start(j, _):
            row = ids[step * group + j]
            pltpu.make_async_copy(emb_ref.at[0, pl.ds(row, 1), :], buf.at[slot, pl.ds(j, 1), :], sems.at[slot]).start()
            return 0

        lax.fori_loop(0, group, start, 0, unroll=8)

        def finish(which, base):
            pltpu.make_async_copy(buf.at[which], buf.at[which], sems.at[which]).wait()
            rows_ref[pl.ds(pl.multiple_of(base, 16), group), :] = buf[which].astype(BF16)

        @pl.when(step > 0)
        def _():
            finish(1 - slot, (step - 1) * group)

        @pl.when(step == n_blocks - 1)
        def _():
            finish(slot, step * group)

    @pl.when(jnp.logical_not(is_first))
    def _():
        @pl.when(step == 0)
        def _():
            acc[...] = jnp.zeros_like(acc)

        lane = lax.broadcasted_iota(jnp.int32, (128, 128), 1)

        def extract(block, base, w_block):
            width = w_block.shape[1]
            begins, counts = [], []
            for side in range(2):
                begin = off[side, block]
                end = off[side, block + 1]
                begin16 = (begin // 16) * 16
                begins.append(begin16)
                counts.append(jnp.where(end > begin, (end - begin16 + 127) // 128, 0))

            def body(it, _):
                starts = [pl.multiple_of(jnp.minimum(b + it * 128, n_pad), 16) for b in begins]
                hot = []
                for side in range(2):
                    rel = tgt_ref[side, pl.ds(starts[side], 128), :] - base
                    hot.append(jnp.concatenate([jnp.where(rel - 128 * j == lane, 1.0, 0.0).astype(BF16) for j in range(width // 128)], axis=1))
                picked = dot_nt(jnp.concatenate(hot, axis=0), w_block[...])
                for side in range(2):
                    acc[side, pl.ds(starts[side], 128), :] += picked[side * 128:(side + 1) * 128]
                return 0

            lax.fori_loop(0, jnp.maximum(counts[0], counts[1]), body, 0)

        extract(step, step * VB, w_ref)

        @pl.when(step == n_blocks - 1)
        def _():
            extract(n_blocks, n_blocks * VB, wt_ref)
            out_ref[...] = acc[:, :n_pad, :].astype(BF16)


def prep(core, ids, off, emb_stack, w_out, w_tail, tgt_wide):
    hidden, vocab = w_out.shape
    n_blocks = vocab // VB
    n_pad = ids.shape[0] // 2
    group = ids.shape[0] // n_blocks
    whole = pl.Buffered(1)

    return pl.pallas_call(
        functools.partial(prep_kernel, group=group, n_pad=n_pad, n_blocks=n_blocks),
        grid_spec=pltpu.PrefetchScalarGridSpec(
            num_scalar_prefetch=3,
            grid=(n_blocks,),
            in_specs=[
                pl.BlockSpec(memory_space=pl.ANY),
                pl.BlockSpec((hidden, VB), lambda v, *_: (0, v)),
                pl.BlockSpec((hidden, TAIL), lambda v, *_: (0, 0), pipeline_mode=whole),
                pl.BlockSpec(tgt_wide.shape, lambda v, *_: (0, 0, 0), pipeline_mode=whole),
            ],
            out_specs=[
                pl.BlockSpec((2 * n_pad, hidden), lambda v, *_: (0, 0)),
                pl.BlockSpec((2, n_pad, hidden), lambda v, *_: (0, 0, 0)),
            ],
            scratch_shapes=[
                pltpu.VMEM((2, group, hidden), F32),
                pltpu.VMEM((2, n_pad + 128, hidden), F32),
                pltpu.SemaphoreType.DMA((2,)),
            ],
        ),
        out_shape=[
            jax.ShapeDtypeStruct((2 * n_pad, hidden), BF16),
            jax.ShapeDtypeStruct((2, n_pad, hidden), BF16),
        ],
        compiler_params=pltpu.CompilerParams(vmem_limit_bytes=48 * 2**20, dimension_semantics=("arbitrary",)),
        cost_estimate=pl.CostEstimate(flops=10**10, bytes_accessed=10**8, transcendentals=0),
        name="prep",
    )(core, ids, off, emb_stack, w_out, w_tail, tgt_wide)


def heads_kernel(x_ref, wt_ref, w_ref, w_any, acc_ref, l_ref, m_ref, s0, s1, p0, p1, sem, *, n_blocks):
    step = pl.program_id(0)
    n_chunks = x_ref.shape[0] // RC

    def rows_of(r):
        return pl.ds(pl.multiple_of(r * RC, RC), RC)

    def logits(r, s_ref):
        s_ref[...] = dot(x_ref[rows_of(r), :], w_ref[...])

    def weights(r, s_ref, p_ref):
        top = m_ref[rows_of(r), :]
        total = l_ref[rows_of(r), :]
        for j in range(VB // 128):
            cols = slice(j * 128, (j + 1) * 128)
            e = jnp.exp2(s_ref[:, cols] * LOG2E - top)
            total = total + e
            p_ref[:, cols] = e.astype(BF16)
        l_ref[rows_of(r), :] = total

    def gather(r, p_ref):
        acc_ref[rows_of(r), :] += dot_nt(p_ref[...], w_ref[...])

    def start_rows(r, _):
        s = dot(x_ref[rows_of(r), :], wt_ref[...]) * LOG2E
        top = jnp.max(s, axis=1, keepdims=True)
        e = jnp.exp2(s - top)
        m_ref[rows_of(r), :] = jnp.broadcast_to(top, (RC, 128))
        l_ref[rows_of(r), :] = e
        acc_ref[rows_of(r), :] = dot_nt(e.astype(BF16), wt_ref[...])
        return 0

    @pl.when(step == 0)
    def _():
        lax.fori_loop(0, n_chunks, start_rows, 0)

    logits(0, s0)

    def pair(i, _):
        r = 2 * i
        logits(r + 1, s1)
        weights(r, s0, p0)
        gather(r, p0)
        logits(lax.rem(r + 2, n_chunks), s0)
        weights(r + 1, s1, p1)
        gather(r + 1, p1)
        return 0

    lax.fori_loop(0, n_chunks // 2, pair, 0)

    @pl.when(step == n_blocks - 1)
    def _():
        top_sum = jnp.max(jnp.where(l_ref[...] < 1e30, 0.0, 1.0))

        @pl.when(top_sum > 0.0)
        def _():
            lax.fori_loop(0, n_chunks, start_rows, 0)

            def block(v, _):
                copy = pltpu.make_async_copy(w_any.at[:, pl.ds(pl.multiple_of(v * VB, VB), VB)], w_ref, sem)
                copy.start()
                copy.wait()

                def redo(r, _):
                    rows = rows_of(r)
                    s = dot(x_ref[rows, :], w_ref[...]) * LOG2E
                    old = m_ref[rows, :]
                    new = jnp.maximum(old, jnp.max(s, axis=1, keepdims=True))
                    shrink = jnp.exp2(old - new)
                    e = jnp.exp2(s - new[:, :1])
                    total = l_ref[rows, :] * shrink
                    for j in range(VB // 128):
                        total = total + e[:, j * 128:(j + 1) * 128]
                    l_ref[rows, :] = total
                    m_ref[rows, :] = new
                    acc_ref[rows, :] = acc_ref[rows, :] * shrink[:, :1] + dot_nt(e.astype(BF16), w_ref[...])
                    return 0

                lax.fori_loop(0, n_chunks, redo, 0)
                return 0

            lax.fori_loop(0, n_blocks, block, 0)


def heads(x, w_out, w_tail):

    rows, hidden = x.shape
    n_blocks = w_out.shape[1] // VB
    whole = pl.Buffered(1)
    fixed = lambda v: (0, 0)
    flops = 4 * rows * hidden * w_out.shape[1]
    return pl.pallas_call(
        functools.partial(heads_kernel, n_blocks=n_blocks),
        grid=(n_blocks,),
        in_specs=[
            pl.BlockSpec((rows, hidden), fixed, pipeline_mode=whole),
            pl.BlockSpec((hidden, TAIL), fixed, pipeline_mode=whole),
            pl.BlockSpec((hidden, VB), lambda v: (0, v)),
            pl.BlockSpec(memory_space=pl.ANY),
        ],
        out_specs=[
            pl.BlockSpec((rows, hidden), fixed),
            pl.BlockSpec((rows, 128), fixed),
            pl.BlockSpec((rows, 128), fixed),
        ],
        out_shape=[
            jax.ShapeDtypeStruct((rows, hidden), F32),
            jax.ShapeDtypeStruct((rows, 128), F32),
            jax.ShapeDtypeStruct((rows, 128), F32),
        ],
        scratch_shapes=[
            pltpu.VMEM((RC, VB), F32),
            pltpu.VMEM((RC, VB), F32),
            pltpu.VMEM((RC, VB), BF16),
            pltpu.VMEM((RC, VB), BF16),
            pltpu.SemaphoreType.DMA,
        ],
        compiler_params=pltpu.CompilerParams(vmem_limit_bytes=60 * 2**20, dimension_semantics=("arbitrary",)),
        cost_estimate=pl.CostEstimate(flops=flops, bytes_accessed=10**8, transcendentals=rows * w_out.shape[1]),
        name="heads",
    )(x, w_tail, w_out, w_out)


def table_kernel(blk, first, n_groups, sched_a, sched_b, src_a, src_b, ids_a, ids_b, out_ref, kbuf, ibuf, sems):
    step = pl.program_id(0)
    count = n_groups[0]
    slot = lax.rem(step, 2)

    def copies(which, group):
        made = []
        for side, (sched, src, ids) in enumerate(((sched_a, src_a, ids_a), (sched_b, src_b, ids_b))):
            for k in range(KW):
                index = sched[group * KW + k]
                to = pl.ds((side * KW + k) * 16, 16)
                from_src = pl.ds(pl.multiple_of(jnp.minimum(index * 16, src.shape[0] - 16), 16), 16)
                from_ids = pl.ds(pl.multiple_of(index * 16, 16), 16)
                made.append(pltpu.make_async_copy(src.at[from_src, :], kbuf.at[which, to, :], sems.at[which]))
                made.append(pltpu.make_async_copy(ids.at[from_ids, :], ibuf.at[which, to, :], sems.at[which]))
        return made

    @pl.when((step == 0) & (count > 0))
    def _():
        for copy in copies(0, 0):
            copy.start()

    @pl.when(step + 1 < count)
    def _():
        for copy in copies(1 - slot, step + 1):
            copy.start()

    @pl.when(first[step] == 1)
    def _():
        out_ref[...] = jnp.zeros_like(out_ref)

    @pl.when(step < count)
    def _():
        pltpu.make_async_copy(kbuf.at[slot], kbuf.at[slot], sems.at[slot]).wait()
        pltpu.make_async_copy(ibuf.at[slot], ibuf.at[slot], sems.at[slot]).wait()
        rel = ibuf[slot] - blk[step] * TB
        lane = lax.broadcasted_iota(jnp.int32, rel.shape, 1)
        hot = jnp.concatenate([jnp.where(rel - 128 * j == lane, 1.0, 0.0).astype(BF16) for j in range(TB // 128)], axis=1)
        out_ref[0] += dot_tn(hot, kbuf[slot])


def table(blk, first, n_groups, sched_a, sched_b, src_a, src_b, ids_a, ids_b, vocab):
    hidden = src_a.shape[1]
    n_steps = blk.shape[0]
    anywhere = pl.BlockSpec(memory_space=pl.ANY)
    return pl.pallas_call(
        table_kernel,
        grid_spec=pltpu.PrefetchScalarGridSpec(
            num_scalar_prefetch=5,
            grid=(n_steps,),
            in_specs=[anywhere] * 4,
            out_specs=pl.BlockSpec((1, TB, hidden), lambda s, blk, *_: (0, blk[s], 0)),
            scratch_shapes=[
                pltpu.VMEM((2, 2 * KW * 16, hidden), BF16),
                pltpu.VMEM((2, 2 * KW * 16, 128), jnp.int32),
                pltpu.SemaphoreType.DMA((2,)),
            ],
        ),
        out_shape=jax.ShapeDtypeStruct((1, vocab, hidden), F32),
        compiler_params=pltpu.CompilerParams(vmem_limit_bytes=48 * 2**20, dimension_semantics=("arbitrary",)),
        cost_estimate=pl.CostEstimate(flops=6 * 10**10, bytes_accessed=2 * 10**8, transcendentals=0),
        name="table",
    )(blk, first, n_groups, sched_a, sched_b, src_a, src_b, ids_a, ids_b)


def plan_table(ids_a, ids_b, vocab, active):
    n_blocks = vocab // TB
    n_lists, n = ids_a.shape
    edges = lax.iota(jnp.int32, n_blocks + 1) * TB
    per_list = n // 16
    counts, starts = [], []
    for ids in (ids_a, ids_b):
        off = jnp.sum((ids[:, None, :] < edges[None, :, None]).astype(jnp.int32), axis=-1)
        begin, end = off[:, :-1], off[:, 1:]
        count = jnp.where(end > begin, (end + 15) // 16 - begin // 16, 0) * active
        counts.append(count.T)
        starts.append((begin // 16 + lax.iota(jnp.int32, n_lists)[:, None] * per_list).T)
    need = jnp.maximum(jnp.sum(counts[0], 1), jnp.sum(counts[1], 1))
    groups = jnp.maximum((need + KW - 1) // KW, 1)
    upto = jnp.sum(jnp.where(lax.iota(jnp.int32, n_blocks)[None, :] <= lax.iota(jnp.int32, n_blocks)[:, None], groups[None, :], 0), 1)
    base = upto - groups
    total = upto[-1]
    max_groups = plan_steps(n_lists, n, vocab)
    g_idx = lax.iota(jnp.int32, max_groups)
    blk = jnp.minimum(jnp.sum((upto[None, :] <= g_idx[:, None]).astype(jnp.int32), 1), n_blocks - 1)
    first = jnp.sum((base[None, :] == g_idx[:, None]).astype(jnp.int32), 1)
    scheds = []
    slots = lax.iota(jnp.int32, max_groups * KW)
    dummy = n_lists * per_list
    lower = (lax.iota(jnp.int32, n_lists)[:, None] < lax.iota(jnp.int32, n_lists)[None, :]).astype(jnp.int32)
    for count, start in zip(counts, starts):
        before = jnp.sum(count[:, :, None] * lower[None], axis=1)
        q = ((base * KW)[:, None] + before).reshape(-1)
        c = count.reshape(-1)
        w = start.reshape(-1)
        rel = slots[:, None] - q[None, :]
        inside = (rel >= 0) & (rel < c[None, :])
        scheds.append(jnp.sum(jnp.where(inside, w[None, :] + rel - dummy, 0), 1) + dummy)
    return blk, first, jnp.reshape(total * active, (1,)), scheds[0], scheds[1]


def plan_steps(n_lists, n, vocab):
    n_blocks = vocab // TB
    return 2 * ((n_lists * (n // 16 + n_blocks)) // KW) + n_blocks


def solution(mesh):
    n_stages = mesh.shape['pp']
    n_replicas = mesh.shape['dp']

    def device_fn(tokens, emb_stack, w_up, w_down, gain_final, gain_hid, gain_emb, gain_mtp, w_proj, u_up, u_down, w_out):
        n_micro, batch_dev, ids_width = tokens.shape
        seq_len = ids_width - 2
        vocab, hidden = emb_stack.shape[1:]
        ffn = w_up.shape[-1]
        n_seq = n_micro * batch_dev
        half = n_seq // 2
        n_pos = half * seq_len
        inv_total = 1.0 / (n_seq * n_replicas * seq_len)
        core = lax.axis_index('pp')
        is_first = core == 0
        n_blocks = vocab // VB
        w_tail = w_out[:, n_blocks * VB:]

        seqs = tokens.reshape(2, half, ids_width)
        span = seq_len + 1
        n_slots = half * span
        per_step = -(-n_slots // (n_blocks * 16)) * 16
        n_pad = per_step * n_blocks
        fill = ((0, 0), (0, n_pad - n_slots))
        emb_ids = jnp.pad(seqs[:, :, :span].reshape(2, n_slots), fill)
        targets = jnp.pad(seqs[:, :, 1:].reshape(2, n_slots), fill, constant_values=vocab)
        t_rank = rank_of(targets)
        t_sorted = sort_by_rank(targets, t_rank)
        edges = jnp.minimum(lax.iota(jnp.int32, n_blocks + 2) * VB, vocab)
        off = jnp.sum((t_sorted[:, None, :] < edges[None, :, None]).astype(jnp.int32), axis=-1)
        tgt_wide = jnp.broadcast_to(jnp.pad(t_sorted, ((0, 0), (0, 128)), constant_values=vocab)[:, :, None], (2, n_pad + 128, 128))

        emb_rows, wt_rows = prep(jnp.reshape(core, (1,)), emb_ids.reshape(-1), off, emb_stack, w_out, w_tail, tgt_wide)
        emb_rows = emb_rows.reshape(2, n_pad, hidden)
        swap = [(0, 1), (1, 0)]
        got = lax.ppermute(jnp.where(is_first, emb_rows[1], wt_rows[0]), 'pp', swap)
        own_emb = jnp.where(is_first, emb_rows[0], got)
        own_wt = jnp.where(is_first, got, wt_rows[1])
        own_rank = jnp.where(is_first, t_rank[0], t_rank[1])
        own_seqs = jnp.where(is_first, seqs[0], seqs[1])

        own_emb = own_emb[:n_slots].reshape(half, span, hidden)
        x0 = own_emb[:, :seq_len].reshape(n_pos, hidden)
        e1 = own_emb[:, 1:].reshape(n_pos, hidden)
        hit = own_rank[:n_slots, None] == lax.iota(jnp.int32, n_pad)[None, :]
        wt_slots = dot(hit.astype(BF16), own_wt).astype(BF16).reshape(half, span, hidden)
        wt_main = wt_slots[:, :seq_len].reshape(n_pos, hidden)
        wt_mtp = wt_slots[:, 1:].reshape(n_pos, hidden)

        up_both = lax.all_gather(w_up[0, 0], 'pp')
        down_both = lax.all_gather(w_down[0, 0], 'pp')
        stage_in = x0
        saved = []
        for stage in range(n_stages):
            normed = rms_plain(stage_in)
            out, pre_act, gelu_out = mlp_forward(stage_in, normed, up_both[stage], down_both[stage])
            saved.append((stage_in, normed, pre_act, gelu_out))
            stage_in = out
        hid = stage_in

        def joined_of(h, e):
            return jnp.concatenate([rms_scale(h, gain_hid), rms_scale(e, gain_emb)], axis=-1)

        feat_main, pull_main = jax.vjp(lambda h: rms_scale(h, gain_final), hid)
        joined, pull_joined = jax.vjp(joined_of, hid, e1)
        mtp_in = dot(joined, w_proj).astype(BF16)
        mtp_normed, pull_mtp = jax.vjp(lambda z: rms_scale(z, gain_mtp), mtp_in)
        mtp_out, mtp_pre, _ = mlp_forward(mtp_in, mtp_normed, u_up, u_down)
        feat_mtp, pull_out = jax.vjp(lambda z: rms_scale(z, gain_final), mtp_out)

        feats = jnp.concatenate([feat_main, feat_mtp])
        acc, sums, tops = heads(feats, w_out, w_tail)
        total = jnp.sum(sums, axis=1, keepdims=True)
        scale = jnp.concatenate([jnp.full((n_pos, 1), inv_total, F32), jnp.full((n_pos, 1), MTP_WEIGHT * inv_total, F32)])
        wt = jnp.concatenate([wt_main, wt_mtp])
        picked = jnp.sum(feats.astype(F32) * wt.astype(F32), axis=1, keepdims=True)
        log_norm = (tops[:, :1] + jnp.log2(total)) * LN2
        loss_part = jnp.sum((log_norm - picked) * scale)
        d_feats = ((acc / total - wt.astype(F32)) * scale).astype(BF16)

        d_mtp_out = pull_out(d_feats[n_pos:])[0]
        _, d_mtp_normed = mlp_backward(d_mtp_out, mtp_pre, u_up, u_down)
        d_mtp_in = add_bf16(d_mtp_out, pull_mtp(d_mtp_normed)[0])
        d_joined = dot_nt(d_mtp_in, w_proj).astype(BF16)
        d_hid, d_e1 = pull_joined(d_joined)
        grad = d_hid + pull_main(d_feats[:n_pos])[0]

        d_ups, d_downs = [], []
        for stage in reversed(range(n_stages)):
            stage_in, normed, pre_act, gelu_out = saved[stage]
            d_downs.append(dot_tn(gelu_out, grad))
            grad_pre, d_normed = mlp_backward(grad, pre_act, up_both[stage], down_both[stage])
            d_ups.append(dot_tn(normed, grad_pre))
            grad = add_bf16(grad, jax.vjp(rms_plain, stage_in)[1](d_normed)[0])

        grad_ids = jnp.stack([own_seqs[:, :seq_len].reshape(n_pos), own_seqs[:, 1:seq_len + 1].reshape(n_pos)])
        g_rank = rank_of(grad_ids)
        g_sorted = sort_by_rank(grad_ids, g_rank)
        mine = jnp.concatenate([sort_rows(grad, g_rank[0]), sort_rows(d_e1, g_rank[1])])
        all_ids = lax.all_gather(lax.all_gather(g_sorted, 'dp'), 'pp').reshape(2, n_replicas * 2, n_pos)
        gathered = lax.all_gather(mine, 'dp', tiled=True)
        other = lax.ppermute(gathered, 'pp', [(1, 0)])
        plan = plan_table(all_ids[0], all_ids[1], vocab, jnp.where(is_first, 1, 0))
        pad_ids = [jnp.pad(a.reshape(-1), (0, 16), constant_values=-1) for a in (all_ids[0], all_ids[1])]
        wide = [jnp.broadcast_to(a[:, None], (a.shape[0], 128)) for a in pad_ids]
        d_table = table(*plan, gathered, other, wide[0], wide[1], vocab)

        d_up = jnp.stack(d_ups[::-1])
        d_down = jnp.stack(d_downs[::-1])
        d_up, d_down, _ = lax.optimization_barrier((d_up, d_down, other[:8]))
        d_up = lax.psum_scatter(d_up, 'pp', scatter_dimension=0, tiled=True)
        d_down = lax.psum_scatter(d_down, 'pp', scatter_dimension=0, tiled=True)
        d_up = lax.psum(d_up, 'dp')
        d_down = lax.psum(d_down, 'dp')
        total_loss = lax.psum(loss_part, ('dp', 'pp'))
        return total_loss, d_table, d_up[None], d_down[None]

    in_specs = (P(None, 'dp', None), P('pp', None, None), P('pp', None, None, None), P('pp', None, None, None), P(None), P(None), P(None), P(None), P(None, None), P(None, None), P(None, None), P(None, None))
    out_specs = (P(), P('pp', None, None), P('pp', None, None, None), P('pp', None, None, None))
    return jax.shard_map(device_fn, mesh=mesh, in_specs=in_specs, out_specs=out_specs, check_vma=False)
```
